32 devices in a mesh: dp: 1 (over z), ep: 32 (over y, x, core).
Axes of the slice: x: 4, y: 4, z: 1, core: 2. Of those that a mesh axis runs over, the one named last changes fastest.
The devices are a block of a 4x4x8 slice.
Arguments:
- tokens: bfloat16 [8192, 1024], P(('dp', 'ep'))
- expert_ids: int32 [8192, 8], P(('dp', 'ep'))
- gate_w: float32 [8192, 8], P(('dp', 'ep'))
- route_counts: int32 [32, 32], P(('dp', 'ep'))
- w_gate: bfloat16 [32, 1024, 512], P('ep')
- w_up: bfloat16 [32, 1024, 512], P('ep')
- w_down: bfloat16 [32, 512, 1024], P('ep')
Outputs:
- output: bfloat16 [8192, 1024], P(('dp', 'ep'))
All inputs are finite; a program needn't handle non-finite values.
Results may differ from the reference program's by a relative error of at most 0.00360921.
Values are sent between devices in bfloat16 or wider.
A program may use at most 768 MiB of HBM per device.

```python
import jax
import jax.numpy as jnp
from jax import lax

GROUP_SIZE = 32
TOKENS_DEV = 256
MODEL_DIM = 1024
FFN_DIM = 512
NUM_EXPERTS = 32
TOP_K = 8
CAPACITY = 128
HOT_DEVS = 4

LOCAL_EXPERTS = NUM_EXPERTS // GROUP_SIZE
GROUP_ROWS = GROUP_SIZE * TOKENS_DEV


def draw_routing(route_key):
    key_hot, key_star, key_noise, key_cover = jax.random.split(route_key, 4)
    expert_ar = jnp.arange(NUM_EXPERTS)
    expert_dev = expert_ar // LOCAL_EXPERTS
    hot_base = jax.random.randint(key_hot, (), 0, GROUP_SIZE)
    hot_list = (hot_base + jnp.arange(HOT_DEVS) * (GROUP_SIZE // HOT_DEVS)) % GROUP_SIZE
    is_hot = jnp.any(expert_dev[:, None] == hot_list[None, :], axis=1)
    star_expert = hot_base * LOCAL_EXPERTS + jax.random.randint(key_star, (), 0, LOCAL_EXPERTS)
    bonus_int = jnp.where(is_hot, 50, 0) + jnp.where(expert_ar == star_expert, 1000, 0)
    noise_int = jax.random.randint(key_noise, (GROUP_SIZE, TOKENS_DEV, NUM_EXPERTS), 0, 100)
    source = jnp.arange(GROUP_SIZE)
    tok_ar = jnp.arange(TOKENS_DEV)
    choice = jnp.arange(TOP_K)
    cover_rank = tok_ar[:, None] * (TOP_K - 1) + choice[None, :] - 1
    forced = (choice[None, :] >= 1) & (cover_rank < GROUP_SIZE - 1)
    cover_dev = (source[:, None, None] + 1 + cover_rank[None, :, :]) % GROUP_SIZE
    cover_exp = cover_dev * LOCAL_EXPERTS + jax.random.randint(key_cover, (GROUP_SIZE, TOKENS_DEV, TOP_K), 0, LOCAL_EXPERTS)
    taken_mask = jnp.any((cover_exp[:, :, :, None] == expert_ar) & forced[None, :, :, None], axis=2)
    home_mask = (expert_dev[None, :] == source[:, None])[:, None, :]
    pick_score = jnp.where(home_mask | taken_mask, -1, noise_int + bonus_int[None, None, :])
    ranked = lax.top_k(pick_score * NUM_EXPERTS + expert_ar, TOP_K)[1]
    n_forced = jnp.sum(forced.astype(jnp.int32), axis=1)
    pick_col = jnp.clip(jnp.where(choice[None, :] == 0, 0, choice[None, :] - n_forced[:, None]), 0, TOP_K - 1)
    free_exp = jnp.take_along_axis(ranked, jnp.broadcast_to(pick_col[None, :, :], ranked.shape), axis=2)
    expert_ids = jnp.where(forced[None, :, :], cover_exp, free_exp).astype(jnp.int32)
    onehot = (expert_ids.reshape(GROUP_SIZE, TOKENS_DEV * TOP_K, 1) == expert_ar).astype(jnp.int32)
    route_counts = jnp.minimum(jnp.sum(onehot, axis=1), CAPACITY).astype(jnp.int32)
    return expert_ids.reshape(GROUP_ROWS, TOP_K), route_counts


def setup_inputs(seed: int = 0, part: int = 0) -> dict:
    base_key = jax.random.key(seed)
    part_key = jax.random.fold_in(base_key, part)
    key_route, key_tok, key_gate = jax.random.split(part_key, 3)
    key_wg, key_wu, key_wd = jax.random.split(jax.random.key(seed + 1), 3)
    expert_ids, route_counts = draw_routing(key_route)
    tokens = jax.random.normal(key_tok, (GROUP_ROWS, MODEL_DIM), jnp.float32).astype(jnp.bfloat16)
    gate_w = jax.nn.softmax(jax.random.normal(key_gate, (GROUP_ROWS, TOP_K), jnp.float32), axis=-1)
    w_gate = (jax.random.normal(key_wg, (NUM_EXPERTS, MODEL_DIM, FFN_DIM), jnp.float32) * MODEL_DIM ** -0.5).astype(jnp.bfloat16)
    w_up = (jax.random.normal(key_wu, (NUM_EXPERTS, MODEL_DIM, FFN_DIM), jnp.float32) * MODEL_DIM ** -0.5).astype(jnp.bfloat16)
    w_down = (jax.random.normal(key_wd, (NUM_EXPERTS, FFN_DIM, MODEL_DIM), jnp.float32) * FFN_DIM ** -0.5).astype(jnp.bfloat16)
    return {"tokens": tokens, "expert_ids": expert_ids, "gate_w": gate_w, "route_counts": route_counts, "w_gate": w_gate, "w_up": w_up, "w_down": w_down}


def reference(tokens, expert_ids, gate_w, route_counts, w_gate, w_up, w_down):
    expert_ar = jnp.arange(NUM_EXPERTS)
    flat_ids = expert_ids.reshape(GROUP_SIZE, TOKENS_DEV * TOP_K)
    onehot = (flat_ids[:, :, None] == expert_ar).astype(jnp.int32)
    before = jnp.cumsum(onehot, axis=1) - onehot
    slot_idx = jnp.sum(before * onehot, axis=2).reshape(GROUP_SIZE, TOKENS_DEV, TOP_K)
    row_limit = jnp.sum(onehot * route_counts[:, None, :], axis=2).reshape(GROUP_SIZE, TOKENS_DEV, TOP_K)
    kept_mask = slot_idx < row_limit
    ids_3d = expert_ids.reshape(GROUP_SIZE, TOKENS_DEV, TOP_K)
    gates_3d = gate_w.reshape(GROUP_SIZE, TOKENS_DEV, TOP_K)
    tok_3d = tokens.reshape(GROUP_SIZE, TOKENS_DEV, MODEL_DIM).astype(jnp.float32)
    slot_hit = slot_idx[:, None, :, :] == jnp.arange(CAPACITY)[None, :, None, None]

    def one_expert(acc_out, blk_args):
        expert_id, gate_mat, up_mat, down_mat = blk_args
        place_mask = slot_hit & ((ids_3d == expert_id) & kept_mask)[:, None, :, :]
        disp_mat = jnp.sum(place_mask.astype(jnp.float32), axis=3)
        comb_w = jnp.sum(jnp.where(place_mask, gates_3d[:, None, :, :], 0.0), axis=3)
        rows_in = jnp.einsum("gct,gtd->gcd", disp_mat, tok_3d).astype(jnp.bfloat16).reshape(GROUP_SIZE * CAPACITY, MODEL_DIM)
        act_a = jnp.dot(rows_in, gate_mat, preferred_element_type=jnp.float32)
        act_b = jnp.dot(rows_in, up_mat, preferred_element_type=jnp.float32)
        hidden = (jax.nn.silu(act_a) * act_b).astype(jnp.bfloat16)
        rows_out = jnp.dot(hidden, down_mat, preferred_element_type=jnp.float32).astype(jnp.bfloat16)
        rows_out = rows_out.reshape(GROUP_SIZE, CAPACITY, MODEL_DIM).astype(jnp.float32)
        return acc_out + jnp.einsum("gct,gcd->gtd", comb_w, rows_out), None

    summed = lax.scan(one_expert, tok_3d, (expert_ar, w_gate, w_up, w_down))[0]
    return summed.astype(jnp.bfloat16).reshape(GROUP_ROWS, MODEL_DIM)
```

```python
import math

import jax
import jax.numpy as jnp
from jax import lax
from jax.experimental import pallas as pl
from jax.experimental.pallas import tpu as pltpu
from jax.sharding import PartitionSpec as P

MESH = pl.DeviceIdType.MESH
CORES = 2
LANES = 128
CHUNKS = (256, 256, 256, 128, 128)
F32 = jnp.float32
BF16 = jnp.bfloat16


def moe_kernel(side, cols, ids_ref, gate_ref, cnt_ref, tok_hbm, wg_hbm, wu_hbm, wd_hbm, out_ref,
               xbuf, gbuf, gsel, wg, wu, hbuf, wd, acc, d2d, tpl, tmi, rpl, rmi,
               send, recv, loc):
    tok_n = tok_hbm.shape[0]
    half_t = tok_n // 2
    ffn = wd_hbm.shape[1]
    half_f = ffn // 2
    n_chunk = len(cols)
    top_n = ids_ref.shape[1]
    opp = side // 2

    me = lax.axis_index("ep")
    core = lax.rem(me, CORES)
    xpos = lax.rem(me // CORES, side)
    ypos = me // (CORES * side)

    def dev(yy, xx, cc):
        return (lax.rem(yy, side) * side + lax.rem(xx, side)) * CORES + cc

    partner = dev(ypos, xpos, 1 - core)
    xp, xm, xo = dev(ypos, xpos + 1, core), dev(ypos, xpos + side - 1, core), dev(ypos, xpos + opp, core)
    yp, ym = dev(ypos + 1, xpos, core), dev(ypos + side - 1, xpos, core)

    barrier = pltpu.get_barrier_semaphore()
    for peer in (partner, xp, xm, xo, yp, ym):
        pl.semaphore_signal(barrier, inc=1, device_id={"ep": peer}, device_id_type=MESH)
    pl.semaphore_wait(barrier, 6)

    count = [0]
    sent = []

    def rcopy(src, dst, peer):
        i = count[0]
        count[0] += 1
        c = pltpu.make_async_remote_copy(src_ref=src, dst_ref=dst, send_sem=send.at[i], recv_sem=recv.at[i],
                                         device_id={"ep": peer}, device_id_type=MESH)
        sent.append(c)
        return c

    lcount = [0]

    def lcopy(src, dst):
        i = lcount[0]
        lcount[0] += 1
        c = pltpu.make_async_copy(src, dst, loc.at[i])
        c.start()
        return c

    tok_in = {0: rcopy(tok_hbm, xbuf.at[0, 1], partner), 3: rcopy(tok_hbm, xbuf.at[3, 0], xp),
              1: rcopy(tok_hbm, xbuf.at[1, 0], xm), 2: rcopy(tok_hbm, xbuf.at[2, 0], xo)}
    wgt_3 = rcopy(wg_hbm.at[0], wg.at[3], yp)
    wup_1 = rcopy(wu_hbm.at[0], wu.at[1], ym)
    wup_3 = rcopy(wu_hbm.at[0], wu.at[3], yp)
    wgt_1 = rcopy(wg_hbm.at[0], wg.at[1], ym)
    tok_in[0].start()
    wgt_3.start()
    wup_1.start()
    for r in (1, 3, 2):
        tok_in[r].start()
    wup_3.start()
    wgt_1.start()
    loc_x = lcopy(tok_hbm, xbuf.at[0, 0])
    loc_g = lcopy(wg_hbm.at[0], wg.at[0])
    loc_u = lcopy(wu_hbm.at[0], wu.at[0])
    loc_d = [lcopy(wd_hbm.at[0, :, pl.ds(c0, cw)], wd[k].at[0]) for k, (c0, cw) in enumerate(cols)]

    lane = lax.broadcasted_iota(jnp.int32, (tok_n, LANES), 1)
    picked = jnp.zeros((tok_n, LANES), F32)
    gates = jnp.zeros((tok_n, LANES), F32)
    for j in range(top_n):
        hit = ids_ref[:, j:j + 1] == lane
        picked = jnp.where(hit, 1.0, picked)
        gates = jnp.where(hit, gate_ref[:, j:j + 1], gates)
    earlier = lax.broadcasted_iota(jnp.int32, (tok_n, tok_n), 1) < lax.broadcasted_iota(jnp.int32, (tok_n, tok_n), 0)
    before = jnp.dot(jnp.where(earlier, 1.0, 0.0).astype(BF16), picked.astype(BF16), preferred_element_type=F32)
    gbuf[0, 0] = jnp.where(before < cnt_ref[0:1, :].astype(F32), gates, 0.0)

    def h_block(slot, r, c):
        x = xbuf[r, c]
        a = jnp.dot(x, wg[slot], preferred_element_type=F32)
        b = jnp.dot(x, wu[slot], preferred_element_type=F32)
        hbuf[slot, r, c] = (a * jax.nn.sigmoid(a) * b).astype(BF16)

    loc_x.wait()
    loc_g.wait()
    loc_u.wait()
    h_block(0, 0, 0)
    gate_in = {0: rcopy(gbuf.at[0, 0], gbuf.at[0, 1], partner), 3: rcopy(gbuf.at[0, 0], gbuf.at[3, 0], xp),
               1: rcopy(gbuf.at[0, 0], gbuf.at[1, 0], xm), 2: rcopy(gbuf.at[0, 0], gbuf.at[2, 0], xo)}
    for r in (0, 1, 3, 2):
        gate_in[r].start()
    tok_in[0].wait_recv()
    h_block(0, 0, 1)
    tok_fwd, gate_fwd = {}, {}
    for r in (1, 3, 2):
        tok_in[r].wait_recv()
        tok_fwd[r] = rcopy(xbuf.at[r, 0], xbuf.at[r, 1], partner)
        tok_fwd[r].start()
        h_block(0, r, 0)
    for r in (1, 3, 2):
        tok_fwd[r].wait_recv()
        h_block(0, r, 1)

    wgt_3.wait_recv()
    wgt_2 = rcopy(wg.at[3], wg.at[2], yp)
    wgt_2.start()
    wup_1.wait_recv()
    wup_2 = rcopy(wu.at[1], wu.at[2], ym)
    wup_2.start()

    own_p, own_m, fwd_p, fwd_m = [], [], [], []
    for k in range(n_chunk):
        loc_d[k].wait()
        own_p.append(rcopy(wd[k].at[0], wd[k].at[3], yp))
        own_m.append(rcopy(wd[k].at[0], wd[k].at[1], ym))
        fwd_p.append(rcopy(wd[k].at[3, pl.ds(0, half_f)], wd[k].at[2, pl.ds(0, half_f)], yp))
        fwd_m.append(rcopy(wd[k].at[1, pl.ds(half_f, half_f)], wd[k].at[2, pl.ds(half_f, half_f)], ym))
    for k in range(2):
        own_p[k].start()
        own_m[k].start()

    gate_in[0].wait_recv()
    for r in (1, 3, 2):
        gate_in[r].wait_recv()
        gate_fwd[r] = rcopy(gbuf.at[r, 0], gbuf.at[r, 1], partner)
        gate_fwd[r].start()

    def h_all(slot):
        def body(i, _):
            h_block(slot, i // CORES, lax.rem(i, CORES))
            return 0
        lax.fori_loop(0, side * CORES, body, 0)

    for r in (1, 3, 2):
        gate_fwd[r].wait_recv()

    def sel_body(i, _):
        g = gbuf[i // CORES, lax.rem(i, CORES)]
        for s in range(side):
            one = jnp.sum(jnp.where(lane == dev(ypos + s, xpos, core), g, 0.0), axis=1, keepdims=True)
            gsel[s, i // CORES, lax.rem(i, CORES)] = jnp.broadcast_to(one, (tok_n, LANES))
        return 0
    lax.fori_loop(0, side * CORES, sel_body, 0)

    wup_3.wait_recv()
    h_all(3)
    wgt_1.wait_recv()
    h_all(1)
    wgt_2.wait_recv()
    wup_2.wait_recv()
    h_all(2)

    def gated(s, r, c, k):
        y = jnp.dot(hbuf[s, r, c], wd[k][s], preferred_element_type=F32).astype(BF16).astype(F32)
        g = gsel[s, r, c]
        return jnp.concatenate([jnp.where(g > 0.0, g * y[:, q:q + LANES], 0.0) for q in range(0, cols[k][1], LANES)], axis=1)

    exch, t_p, t_m, r_p, r_m = [], [], [], [], []

    def stage_a(k):
        own_p[k].wait_recv()
        fwd_p[k].start()
        own_m[k].wait_recv()
        fwd_m[k].start()
        if k + 2 < n_chunk:
            own_p[k + 2].start()
            own_m[k + 2].start()

        def first(i, _):
            r, c = i // CORES, lax.rem(i, CORES)
            acc[k][c, r] = gated(0, r, c, k) + gated(1, r, c, k) + gated(3, r, c, k)
            return 0
        lax.fori_loop(0, side * CORES, first, 0)
        fwd_p[k].wait_recv()
        fwd_m[k].wait_recv()

        def last(i, _):
            r, c = lax.rem(i, side), 1 - i // side
            acc[k][c, r] = acc[k][c, r] + gated(2, r, c, k)
            return 0
        lax.fori_loop(0, side, last, 0)
        exch.append(rcopy(acc[k].at[1], d2d[k], partner))
        exch[k].start()
        lax.fori_loop(side, side * CORES, last, 0)

    def stage_b(k):
        exch[k].wait_recv()
        acc[k][0, 2] = acc[k][0, 2] + d2d[k][2]
        t_p.append(rcopy(acc[k].at[0, 2, pl.ds(0, half_t)], tpl[k], xp))
        t_m.append(rcopy(acc[k].at[0, 2, pl.ds(half_t, half_t)], tmi[k], xm))
        t_p[k].start()
        t_m[k].start()
        for r in (1, 3, 0):
            acc[k][0, r] = acc[k][0, r] + d2d[k][r]

    def stage_c(k):
        t_p[k].wait_recv()
        acc[k][0, 1, pl.ds(0, half_t)] = acc[k][0, 1, pl.ds(0, half_t)] + tpl[k][...]
        r_p.append(rcopy(acc[k].at[0, 1], rpl[k], xp))
        r_p[k].start()
        t_m[k].wait_recv()
        acc[k][0, 3, pl.ds(half_t, half_t)] = acc[k][0, 3, pl.ds(half_t, half_t)] + tmi[k][...]
        r_m.append(rcopy(acc[k].at[0, 3], rmi[k], xm))
        r_m[k].start()

    def stage_d(k):
        r_p[k].wait_recv()
        r_m[k].wait_recv()
        c0, cw = cols[k]
        total = xbuf[0, 0, :, c0:c0 + cw].astype(F32) + acc[k][0, 0]
        out_ref[:, c0:c0 + cw] = (total + rpl[k][...] + rmi[k][...]).astype(BF16)

    for k in range(n_chunk):
        stage_a(k)
        stage_b(k)
        if k >= 1:
            stage_c(k - 1)
        if k >= 2:
            stage_d(k - 2)
    stage_c(n_chunk - 1)
    if n_chunk >= 2:
        stage_d(n_chunk - 2)
    stage_d(n_chunk - 1)
    for c in sent:
        c.wait_send()


def solution(mesh):
    group_size = mesh.shape["ep"]
    side = math.isqrt(group_size // CORES)
    row_spec = P(("dp", "ep"))

    def local_step(tokens, expert_ids, gate_w, route_counts, w_gate, w_up, w_down):
        tok_n, dim = tokens.shape
        ffn = w_gate.shape[2]
        widths = CHUNKS if sum(CHUNKS) == dim else (LANES,) * (dim // LANES)
        cols = tuple((sum(widths[:k]), cw) for k, cw in enumerate(widths))
        counts = jnp.pad(route_counts, ((0, 0), (0, LANES - route_counts.shape[1])))
        n_copy = 4 + 4 + 4 + 3 + 3 + 2 + 9 * len(cols)
        vmem = pl.BlockSpec(memory_space=pltpu.VMEM)
        anym = pl.BlockSpec(memory_space=pl.ANY)
        return pl.pallas_call(
            lambda *refs: call_kernel(side, cols, refs),
            out_shape=jax.ShapeDtypeStruct((tok_n, dim), BF16),
            in_specs=[vmem] * 3 + [anym] * 4,
            out_specs=vmem,
            scratch_shapes=[
                pltpu.VMEM((side, CORES, tok_n, dim), BF16),
                pltpu.VMEM((side, CORES, tok_n, LANES), F32),
                pltpu.VMEM((side, side, CORES, tok_n, LANES), F32),
                pltpu.VMEM((side, dim, ffn), BF16),
                pltpu.VMEM((side, dim, ffn), BF16),
                pltpu.VMEM((side, side, CORES, tok_n, ffn), BF16),
                [pltpu.VMEM((side, ffn, cw), BF16) for _, cw in cols],
                [pltpu.VMEM((CORES, side, tok_n, cw), F32) for _, cw in cols],
                [pltpu.VMEM((side, tok_n, cw), F32) for _, cw in cols],
                [pltpu.VMEM((tok_n // 2, cw), F32) for _, cw in cols],
                [pltpu.VMEM((tok_n // 2, cw), F32) for _, cw in cols],
                [pltpu.VMEM((tok_n, cw), F32) for _, cw in cols],
                [pltpu.VMEM((tok_n, cw), F32) for _, cw in cols],
                pltpu.SemaphoreType.DMA((n_copy,)),
                pltpu.SemaphoreType.DMA((n_copy,)),
                pltpu.SemaphoreType.DMA((3 + len(cols),)),
            ],
            compiler_params=pltpu.CompilerParams(collective_id=0, has_side_effects=True, vmem_limit_bytes=60 * 2 ** 20),
            name="moe_kernel",
        )(expert_ids, gate_w, counts, tokens, w_gate, w_up, w_down)

    def call_kernel(side, cols, refs):
        moe_kernel(side, cols, *refs)

    return jax.shard_map(local_step, mesh=mesh, in_specs=(row_spec, row_spec, row_spec, row_spec, P("ep"), P("ep"), P("ep")), out_specs=row_spec, check_vma=False)
```

```python
import math

import jax
import jax.numpy as jnp
from jax import lax
from jax.experimental import pallas as pl
from jax.experimental.pallas import tpu as pltpu
from jax.sharding import PartitionSpec as P

MESH = pl.DeviceIdType.MESH
CORES = 2
LANES = 128
CHUNKS = (128,) * 8
AHEAD = 2
PIECES = 2
F32 = jnp.float32
BF16 = jnp.bfloat16


def moe_kernel(side, cols, ids_ref, gate_ref, cnt_ref, tok_hbm, wg_hbm, wu_hbm, wd_hbm, out_ref,
               xbuf, gbuf, gsel, wg, wu, hbuf, wd, acc, d2d, tpl, tmi, rpl, rmi,
               send, recv, loc):
    tok_n = tok_hbm.shape[0]
    half_t = tok_n // 2
    ffn = wd_hbm.shape[1]
    half_f = ffn // 2
    n_chunk = len(cols)
    top_n = ids_ref.shape[0]
    opp = side // 2

    me = lax.axis_index("ep")
    core = lax.rem(me, CORES)
    xpos = lax.rem(me // CORES, side)
    ypos = me // (CORES * side)

    def dev(yy, xx, cc):
        return (lax.rem(yy, side) * side + lax.rem(xx, side)) * CORES + cc

    partner = dev(ypos, xpos, 1 - core)
    xp, xm, xo = dev(ypos, xpos + 1, core), dev(ypos, xpos + side - 1, core), dev(ypos, xpos + opp, core)
    yp, ym = dev(ypos + 1, xpos, core), dev(ypos + side - 1, xpos, core)

    barrier = pltpu.get_barrier_semaphore()
    for peer in (partner, xp, xm, xo, yp, ym):
        pl.semaphore_signal(barrier, inc=1, device_id={"ep": peer}, device_id_type=MESH)
    pl.semaphore_wait(barrier, 6)

    count = [0]
    sent = []

    def rcopy(src, dst, peer):
        i = count[0]
        count[0] += 1
        c = pltpu.make_async_remote_copy(src_ref=src, dst_ref=dst, send_sem=send.at[i], recv_sem=recv.at[i],
                                         device_id={"ep": peer}, device_id_type=MESH)
        sent.append(c)
        return c

    lcount = [0]

    def lcopy(src, dst):
        i = lcount[0]
        lcount[0] += 1
        c = pltpu.make_async_copy(src, dst, loc.at[i])
        c.start()
        return c

    tok_in = {0: rcopy(tok_hbm, xbuf.at[0, 1], partner), 3: rcopy(tok_hbm, xbuf.at[3, 0], xp),
              1: rcopy(tok_hbm, xbuf.at[1, 0], xm)}
    wgt_3 = rcopy(wg_hbm.at[0], wg.at[3], yp)
    wup_1 = rcopy(wu_hbm.at[0], wu.at[1], ym)
    wup_3 = rcopy(wu_hbm.at[0], wu.at[3], yp)
    wgt_1 = rcopy(wg_hbm.at[0], wg.at[1], ym)
    tok_in[0].start()
    wgt_3.start()
    wup_1.start()
    for r in (1, 3):
        tok_in[r].start()
    wup_3.start()
    wgt_1.start()
    loc_x = lcopy(tok_hbm, xbuf.at[0, 0])
    loc_g = lcopy(wg_hbm.at[0], wg.at[0])
    loc_u = lcopy(wu_hbm.at[0], wu.at[0])
    loc_d = [lcopy(wd_hbm.at[0, :, pl.ds(c0, cw)], wd[k].at[0]) for k, (c0, cw) in enumerate(cols)]

    own_p, own_m, fwd_p, fwd_m = [], [], [], []
    for k in range(n_chunk):
        own_p.append(rcopy(wd[k].at[0], wd[k].at[3], yp))
        own_m.append(rcopy(wd[k].at[0], wd[k].at[1], ym))
        fwd_p.append(rcopy(wd[k].at[3, pl.ds(0, half_f)], wd[k].at[2, pl.ds(0, half_f)], yp))
        fwd_m.append(rcopy(wd[k].at[1, pl.ds(half_f, half_f)], wd[k].at[2, pl.ds(half_f, half_f)], ym))
    for k in range(n_chunk):
        loc_d[k].wait()
    for k in range(min(AHEAD, n_chunk)):
        own_p[k].start()
        own_m[k].start()

    n_exp = cnt_ref.shape[1]
    row = lax.broadcasted_iota(jnp.int32, (n_exp, tok_n), 0)
    picked = jnp.zeros((n_exp, tok_n), F32)
    gates = jnp.zeros((n_exp, tok_n), F32)
    for j in range(top_n):
        hit = ids_ref[j:j + 1, :] == row
        picked = jnp.where(hit, 1.0, picked)
        gates = jnp.where(hit, gate_ref[j:j + 1, :], gates)
    earlier = lax.broadcasted_iota(jnp.int32, (tok_n, tok_n), 0) < lax.broadcasted_iota(jnp.int32, (tok_n, tok_n), 1)
    before = jnp.dot(picked.astype(BF16), jnp.where(earlier, 1.0, 0.0).astype(BF16), preferred_element_type=F32)
    limit = jnp.transpose(jnp.broadcast_to(cnt_ref[0:1, :].astype(F32), (8, n_exp)))[:, 0:1]
    gbuf[0, 0] = jnp.where(before < limit, gates, 0.0)

    def h_block(slot, r, c):
        x = xbuf[r, c]
        a = jnp.dot(x, wg[slot], preferred_element_type=F32)
        b = jnp.dot(x, wu[slot], preferred_element_type=F32)
        hbuf[slot, r, c] = (a * jax.nn.sigmoid(a) * b).astype(BF16)

    loc_x.wait()
    loc_g.wait()
    loc_u.wait()
    h_block(0, 0, 0)
    gate_in = {0: rcopy(gbuf.at[0, 0], gbuf.at[0, 1], partner), 3: rcopy(gbuf.at[0, 0], gbuf.at[3, 0], xp),
               1: rcopy(gbuf.at[0, 0], gbuf.at[1, 0], xm), 2: rcopy(gbuf.at[0, 0], gbuf.at[2, 0], xo)}
    for r in (0, 1, 3, 2):
        gate_in[r].start()
    tok_in[0].wait_recv()
    h_block(0, 0, 1)
    tok_fwd, gate_fwd = {}, {}
    lo_t, hi_t = pl.ds(0, half_t), pl.ds(half_t, half_t)
    tok_in[3].wait_recv()
    tok_fwd[3] = rcopy(xbuf.at[3, 0], xbuf.at[3, 1], partner)
    tok_2p = rcopy(xbuf.at[3, 0, lo_t], xbuf.at[2, 0, lo_t], xp)
    tok_2p.start()
    tok_fwd[3].start()
    tok_in[1].wait_recv()
    tok_fwd[1] = rcopy(xbuf.at[1, 0], xbuf.at[1, 1], partner)
    tok_2m = rcopy(xbuf.at[1, 0, hi_t], xbuf.at[2, 0, hi_t], xm)
    tok_2m.start()
    tok_fwd[1].start()
    h_block(0, 3, 0)
    h_block(0, 1, 0)
    tok_fwd[3].wait_recv()
    h_block(0, 3, 1)
    tok_fwd[1].wait_recv()
    h_block(0, 1, 1)
    tok_2p.wait_recv()
    tok_2m.wait_recv()
    tok_fwd[2] = rcopy(xbuf.at[2, 0], xbuf.at[2, 1], partner)
    tok_fwd[2].start()
    h_block(0, 2, 0)
    tok_fwd[2].wait_recv()
    h_block(0, 2, 1)

    pieces = [pl.ds(q * ffn // PIECES, ffn // PIECES) for q in range(PIECES)]
    wgt_3.wait_recv()
    wgt_2 = [rcopy(wg.at[3, :, q], wg.at[2, :, q], yp) for q in pieces]
    for w in wgt_2:
        w.start()
    wup_1.wait_recv()
    wup_2 = [rcopy(wu.at[1, :, q], wu.at[2, :, q], ym) for q in pieces]
    for w in wup_2:
        w.start()

    gate_in[0].wait_recv()
    for r in (1, 3, 2):
        gate_in[r].wait_recv()
        gate_fwd[r] = rcopy(gbuf.at[r, 0], gbuf.at[r, 1], partner)
        gate_fwd[r].start()

    def h_all(slot, q):
        def body(r, _):
            x = xbuf[r].reshape(CORES * tok_n, xbuf.shape[3])
            a = jnp.dot(x, wg[slot, :, q], preferred_element_type=F32)
            b = jnp.dot(x, wu[slot, :, q], preferred_element_type=F32)
            hbuf[slot, r, :, :, q] = (a * jax.nn.sigmoid(a) * b).astype(BF16).reshape(CORES, tok_n, a.shape[1])
            return 0
        lax.fori_loop(0, side, body, 0)

    for r in (1, 3, 2):
        gate_fwd[r].wait_recv()

    lane = lax.broadcasted_iota(jnp.int32, (tok_n, n_exp), 1)

    def sel_body(i, _):
        g = jnp.transpose(gbuf[i // CORES, lax.rem(i, CORES)])
        for s in range(side):
            one = jnp.sum(jnp.where(lane == dev(ypos + s, xpos, core), g, 0.0), axis=1, keepdims=True)
            gsel[s, i // CORES, lax.rem(i, CORES)] = jnp.broadcast_to(one, (tok_n, LANES))
        return 0
    lax.fori_loop(0, side * CORES, sel_body, 0)

    wup_3.wait_recv()
    h_all(3, pl.ds(0, ffn))
    wgt_1.wait_recv()
    h_all(1, pl.ds(0, ffn))

    def gated(s, r, k):
        y = jnp.dot(hbuf[s, r].reshape(CORES * tok_n, ffn), wd[k][s], preferred_element_type=F32).astype(BF16).astype(F32)
        g = gsel[s, r].reshape(CORES * tok_n, LANES)
        z = [jnp.where(g > 0.0, g * y[:, q:q + LANES], 0.0) for q in range(0, cols[k][1], LANES)]
        return jnp.concatenate(z, axis=1).reshape(CORES, tok_n, cols[k][1])

    far, t_p, t_m, r_p, r_m, near = [], [], [], [], [], []

    def place(i):
        return jnp.where(i == 0, 2, jnp.where(i == 1, 1, jnp.where(i == 2, 3, 0)))

    def forward(k):
        own_p[k].wait_recv()
        fwd_p[k].start()
        own_m[k].wait_recv()
        fwd_m[k].start()
        if k + AHEAD < n_chunk:
            own_p[k + AHEAD].start()
            own_m[k + AHEAD].start()

    def first(k):
        def body(i, _):
            r = place(i)
            acc[k][:, i] = gated(0, r, k) + gated(1, r, k) + gated(3, r, k)
            return 0
        lax.fori_loop(0, side, body, 0)

    def last(k):
        fwd_p[k].wait_recv()
        fwd_m[k].wait_recv()
        acc[k][:, 0] = acc[k][:, 0] + gated(2, 2, k)
        far.append(rcopy(acc[k].at[1, pl.ds(0, 1)], d2d[k].at[pl.ds(0, 1)], partner))
        far[k].start()
        for i, r in ((1, 1), (2, 3), (3, 0)):
            acc[k][:, i] = acc[k][:, i] + gated(2, r, k)
        near.append(rcopy(acc[k].at[1, pl.ds(1, side - 1)], d2d[k].at[pl.ds(1, side - 1)], partner))
        near[k].start()

    def stage_b(k):
        far[k].wait_recv()
        acc[k][0, 0] = acc[k][0, 0] + d2d[k][0]
        t_p.append(rcopy(acc[k].at[0, 0, lo_t], tpl[k], xp))
        t_m.append(rcopy(acc[k].at[0, 0, hi_t], tmi[k], xm))
        t_p[k].start()
        t_m[k].start()
        near[k].wait_recv()
        for i in range(1, side):
            acc[k][0, i] = acc[k][0, i] + d2d[k][i]

    def stage_c(k):
        t_p[k].wait_recv()
        acc[k][0, 1, lo_t] = acc[k][0, 1, lo_t] + tpl[k][...]
        r_p.append(rcopy(acc[k].at[0, 1], rpl[k], xp))
        r_p[k].start()
        t_m[k].wait_recv()
        acc[k][0, 2, hi_t] = acc[k][0, 2, hi_t] + tmi[k][...]
        r_m.append(rcopy(acc[k].at[0, 2], rmi[k], xm))
        r_m[k].start()

    def stage_d(k):
        r_p[k].wait_recv()
        r_m[k].wait_recv()
        c0, cw = cols[k]
        total = xbuf[0, 0, :, c0:c0 + cw].astype(F32) + acc[k][0, 3]
        out_ref[:, c0:c0 + cw] = (total + rpl[k][...] + rmi[k][...]).astype(BF16)

    for k in range(min(2, n_chunk)):
        forward(k)
    first(0)
    for p, q in enumerate(pieces):
        wgt_2[p].wait_recv()
        wup_2[p].wait_recv()
        h_all(2, q)
        if p == 0 and n_chunk > 1:
            first(1)
    for k in range(n_chunk):
        last(k)
        if k >= 1 and k + 1 < n_chunk:
            first(k + 1)
        stage_b(k)
        if k >= 1:
            stage_c(k - 1)
        if k + 2 < n_chunk:
            forward(k + 2)
        if k >= 2:
            stage_d(k - 2)
    stage_c(n_chunk - 1)
    for k in range(max(n_chunk - 2, 0), n_chunk):
        stage_d(k)
    for c in sent:
        c.wait_send()


def solution(mesh):
    group_size = mesh.shape["ep"]
    side = math.isqrt(group_size // CORES)
    row_spec = P(("dp", "ep"))

    def local_step(tokens, expert_ids, gate_w, route_counts, w_gate, w_up, w_down):
        tok_n, dim = tokens.shape
        ffn = w_gate.shape[2]
        n_exp = route_counts.shape[1]
        widths = CHUNKS if sum(CHUNKS) == dim else (LANES,) * (dim // LANES)
        cols = tuple((sum(widths[:k]), cw) for k, cw in enumerate(widths))
        n_copy = 5 + 4 + 4 + 3 + 3 + 2 * PIECES + 10 * len(cols)
        vmem = pl.BlockSpec(memory_space=pltpu.VMEM)
        anym = pl.BlockSpec(memory_space=pl.ANY)
        return pl.pallas_call(
            lambda *refs: call_kernel(side, cols, refs),
            out_shape=jax.ShapeDtypeStruct((tok_n, dim), BF16),
            in_specs=[vmem] * 3 + [anym] * 4,
            out_specs=vmem,
            scratch_shapes=[
                pltpu.VMEM((side, CORES, tok_n, dim), BF16),
                pltpu.VMEM((side, CORES, n_exp, tok_n), F32),
                pltpu.VMEM((side, side, CORES, tok_n, LANES), F32),
                pltpu.VMEM((side, dim, ffn), BF16),
                pltpu.VMEM((side, dim, ffn), BF16),
                pltpu.VMEM((side, side, CORES, tok_n, ffn), BF16),
                [pltpu.VMEM((side, ffn, cw), BF16) for _, cw in cols],
                [pltpu.VMEM((CORES, side, tok_n, cw), F32) for _, cw in cols],
                [pltpu.VMEM((side, tok_n, cw), F32) for _, cw in cols],
                [pltpu.VMEM((tok_n // 2, cw), F32) for _, cw in cols],
                [pltpu.VMEM((tok_n // 2, cw), F32) for _, cw in cols],
                [pltpu.VMEM((tok_n, cw), F32) for _, cw in cols],
                [pltpu.VMEM((tok_n, cw), F32) for _, cw in cols],
                pltpu.SemaphoreType.DMA((n_copy,)),
                pltpu.SemaphoreType.DMA((n_copy,)),
                pltpu.SemaphoreType.DMA((3 + len(cols),)),
            ],
            compiler_params=pltpu.CompilerParams(collective_id=0, has_side_effects=True, vmem_limit_bytes=60 * 2 ** 20),
            name="moe_kernel",
        )(expert_ids.T, gate_w.T, route_counts, tokens, w_gate, w_up, w_down)

    def call_kernel(side, cols, refs):
        moe_kernel(side, cols, *refs)

    return jax.shard_map(local_step, mesh=mesh, in_specs=(row_spec, row_spec, row_spec, row_spec, P("ep"), P("ep"), P("ep")), out_specs=row_spec, check_vma=False)
```

```python
import math

import jax
import jax.numpy as jnp
from jax import lax
from jax.experimental import pallas as pl
from jax.experimental.pallas import tpu as pltpu
from jax.sharding import PartitionSpec as P

MESH = pl.DeviceIdType.MESH
CORES = 2
LANES = 128
CHUNKS = (128,) * 8
PIECES = 2
MID = 1
F32 = jnp.float32
BF16 = jnp.bfloat16


def moe_kernel(side, cols, ids_ref, gate_ref, cnt_ref, tok_hbm, wg_hbm, wu_hbm, wd_hbm, out_ref,
               xbuf, gbuf, gsel, wg, wu, hbuf, wd, acc, d2d, tpl, tmi, rpl, rmi,
               send, recv, loc):
    tok_n = tok_hbm.shape[0]
    half_t = tok_n // 2
    ffn = wd_hbm.shape[1]
    half_f = ffn // 2
    n_chunk = len(cols)
    top_n = ids_ref.shape[0]
    opp = side // 2

    me = lax.axis_index("ep")
    core = lax.rem(me, CORES)
    xpos = lax.rem(me // CORES, side)
    ypos = me // (CORES * side)

    def dev(yy, xx, cc):
        return (lax.rem(yy, side) * side + lax.rem(xx, side)) * CORES + cc

    partner = dev(ypos, xpos, 1 - core)
    xp, xm, xo = dev(ypos, xpos + 1, core), dev(ypos, xpos + side - 1, core), dev(ypos, xpos + opp, core)
    yp, ym = dev(ypos + 1, xpos, core), dev(ypos + side - 1, xpos, core)

    barrier = pltpu.get_barrier_semaphore()
    for peer in (partner, xp, xm, xo, yp, ym):
        pl.semaphore_signal(barrier, inc=1, device_id={"ep": peer}, device_id_type=MESH)
    pl.semaphore_wait(barrier, 6)

    count = [0]
    sent = []

    def rcopy(src, dst, peer):
        i = count[0]
        count[0] += 1
        c = pltpu.make_async_remote_copy(src_ref=src, dst_ref=dst, send_sem=send.at[i], recv_sem=recv.at[i],
                                         device_id={"ep": peer}, device_id_type=MESH)
        sent.append(c)
        return c

    lcount = [0]

    def lcopy(src, dst):
        i = lcount[0]
        lcount[0] += 1
        c = pltpu.make_async_copy(src, dst, loc.at[i])
        c.start()
        return c

    tok_in = {0: rcopy(tok_hbm, xbuf.at[0, 1], partner), 3: rcopy(tok_hbm, xbuf.at[3, 0], xp),
              1: rcopy(tok_hbm, xbuf.at[1, 0], xm)}
    wgt_3 = rcopy(wg_hbm.at[0], wg.at[3], yp)
    wup_1 = rcopy(wu_hbm.at[0], wu.at[1], ym)
    wup_3 = rcopy(wu_hbm.at[0], wu.at[3], yp)
    wgt_1 = rcopy(wg_hbm.at[0], wg.at[1], ym)
    tok_in[0].start()
    wgt_3.start()
    wup_1.start()
    for r in (1, 3):
        tok_in[r].start()
    wup_3.start()
    wgt_1.start()
    loc_x = lcopy(tok_hbm, xbuf.at[0, 0])
    loc_g = lcopy(wg_hbm.at[0], wg.at[0])
    loc_u = lcopy(wu_hbm.at[0], wu.at[0])
    loc_d = [lcopy(wd_hbm.at[0, :, pl.ds(c0, cw)], wd[k].at[0]) for k, (c0, cw) in enumerate(cols)]

    lo_f, hi_f = pl.ds(0, half_f), pl.ds(half_f, half_f)
    lead, rest, hop = [], [], []
    for k in range(n_chunk):
        lead.append((rcopy(wd[k].at[0, lo_f], wd[k].at[3, lo_f], yp), rcopy(wd[k].at[0, hi_f], wd[k].at[1, hi_f], ym)))
        rest.append((rcopy(wd[k].at[0, hi_f], wd[k].at[3, hi_f], yp), rcopy(wd[k].at[0, lo_f], wd[k].at[1, lo_f], ym)))
        hop.append((rcopy(wd[k].at[3, lo_f], wd[k].at[2, lo_f], yp), rcopy(wd[k].at[1, hi_f], wd[k].at[2, hi_f], ym)))

    def start(copies):
        for c in copies:
            c.start()

    def arrive(copies):
        for c in copies:
            c.wait_recv()

    for k in range(n_chunk):
        loc_d[k].wait()
    start(lead[0])
    start(rest[0])
    if n_chunk > 1:
        start(lead[1])

    n_exp = cnt_ref.shape[1]
    row = lax.broadcasted_iota(jnp.int32, (n_exp, tok_n), 0)
    picked = jnp.zeros((n_exp, tok_n), F32)
    gates = jnp.zeros((n_exp, tok_n), F32)
    for j in range(top_n):
        hit = ids_ref[j:j + 1, :] == row
        picked = jnp.where(hit, 1.0, picked)
        gates = jnp.where(hit, gate_ref[j:j + 1, :], gates)
    earlier = lax.broadcasted_iota(jnp.int32, (tok_n, tok_n), 0) < lax.broadcasted_iota(jnp.int32, (tok_n, tok_n), 1)
    before = jnp.dot(picked.astype(BF16), jnp.where(earlier, 1.0, 0.0).astype(BF16), preferred_element_type=F32)
    limit = jnp.transpose(jnp.broadcast_to(cnt_ref[0:1, :].astype(F32), (8, n_exp)))[:, 0:1]
    gbuf[0, 0] = jnp.where(before < limit, gates, 0.0)

    def h_block(slot, r, c):
        x = xbuf[r, c]
        a = jnp.dot(x, wg[slot], preferred_element_type=F32)
        b = jnp.dot(x, wu[slot], preferred_element_type=F32)
        hbuf[slot, r, c] = (a * jax.nn.sigmoid(a) * b).astype(BF16)

    loc_x.wait()
    loc_g.wait()
    loc_u.wait()
    h_block(0, 0, 0)
    gate_in = {0: rcopy(gbuf.at[0, 0], gbuf.at[0, 1], partner), 3: rcopy(gbuf.at[0, 0], gbuf.at[3, 0], xp),
               1: rcopy(gbuf.at[0, 0], gbuf.at[1, 0], xm), 2: rcopy(gbuf.at[0, 0], gbuf.at[2, 0], xo)}
    for r in (0, 1, 3, 2):
        gate_in[r].start()
    tok_in[0].wait_recv()
    h_block(0, 0, 1)
    tok_fwd, gate_fwd = {}, {}
    lo_t, hi_t = pl.ds(0, half_t), pl.ds(half_t, half_t)
    tok_in[3].wait_recv()
    tok_fwd[3] = rcopy(xbuf.at[3, 0], xbuf.at[3, 1], partner)
    tok_2p = rcopy(xbuf.at[3, 0, lo_t], xbuf.at[2, 0, lo_t], xp)
    tok_2p.start()
    tok_fwd[3].start()
    tok_in[1].wait_recv()
    tok_fwd[1] = rcopy(xbuf.at[1, 0], xbuf.at[1, 1], partner)
    tok_2m = rcopy(xbuf.at[1, 0, hi_t], xbuf.at[2, 0, hi_t], xm)
    tok_2m.start()
    tok_fwd[1].start()
    h_block(0, 3, 0)
    h_block(0, 1, 0)
    tok_fwd[3].wait_recv()
    h_block(0, 3, 1)
    tok_fwd[1].wait_recv()
    h_block(0, 1, 1)
    tok_2p.wait_recv()
    tok_2m.wait_recv()
    tok_fwd[2] = rcopy(xbuf.at[2, 0], xbuf.at[2, 1], partner)
    tok_fwd[2].start()
    h_block(0, 2, 0)
    tok_fwd[2].wait_recv()
    h_block(0, 2, 1)

    pieces = [pl.ds(q * ffn // PIECES, ffn // PIECES) for q in range(PIECES)]
    wgt_3.wait_recv()
    wgt_2 = [rcopy(wg.at[3, :, q], wg.at[2, :, q], yp) for q in pieces]
    for w in wgt_2:
        w.start()
    wup_1.wait_recv()
    wup_2 = [rcopy(wu.at[1, :, q], wu.at[2, :, q], ym) for q in pieces]
    for w in wup_2:
        w.start()

    gate_in[0].wait_recv()
    for r in (1, 3, 2):
        gate_in[r].wait_recv()
        gate_fwd[r] = rcopy(gbuf.at[r, 0], gbuf.at[r, 1], partner)
        gate_fwd[r].start()

    def h_row(slot, r, q):
        x = xbuf[r].reshape(CORES * tok_n, xbuf.shape[3])
        a = jnp.dot(x, wg[slot, :, q], preferred_element_type=F32)
        b = jnp.dot(x, wu[slot, :, q], preferred_element_type=F32)
        hbuf[slot, r, :, :, q] = (a * jax.nn.sigmoid(a) * b).astype(BF16).reshape(CORES, tok_n, a.shape[1])

    def h_all(slot, q):
        def body(r, _):
            h_row(slot, r, q)
            return 0
        lax.fori_loop(0, side, body, 0)

    for r in (1, 3, 2):
        gate_fwd[r].wait_recv()

    lane = lax.broadcasted_iota(jnp.int32, (tok_n, n_exp), 1)

    def sel_body(i, _):
        g = jnp.transpose(gbuf[i // CORES, lax.rem(i, CORES)])
        for s in range(side):
            one = jnp.sum(jnp.where(lane == dev(ypos + s, xpos, core), g, 0.0), axis=1, keepdims=True)
            gsel[s, i // CORES, lax.rem(i, CORES)] = jnp.broadcast_to(one, (tok_n, LANES))
        return 0
    lax.fori_loop(0, side * CORES, sel_body, 0)

    wup_3.wait_recv()
    h_all(3, pl.ds(0, ffn))
    wgt_1.wait_recv()
    h_all(1, pl.ds(0, ffn))

    def gated(s, r, k):
        y = jnp.dot(hbuf[s, r].reshape(CORES * tok_n, ffn), wd[k][s], preferred_element_type=F32).astype(BF16).astype(F32)
        g = gsel[s, r].reshape(CORES * tok_n, LANES)
        z = [jnp.where(g > 0.0, g * y[:, q:q + LANES], 0.0) for q in range(0, cols[k][1], LANES)]
        return jnp.concatenate(z, axis=1).reshape(CORES, tok_n, cols[k][1])

    far, t_p, t_m, r_p, r_m, near = [], [], [], [], [], []

    def place(i):
        return jnp.where(i == 0, 2, jnp.where(i == 1, 1, jnp.where(i == 2, 3, 0)))

    def forward(k):
        for c, f in zip(lead[k], hop[k]):
            c.wait_recv()
            f.start()
        if k + 1 < n_chunk:
            start(rest[k + 1])
        if k + 2 < n_chunk:
            start(lead[k + 2])

    def first(k, begin, end):
        if begin == 0:
            arrive(rest[k])

        def body(i, _):
            r = place(i)
            acc[k][:, i] = gated(0, r, k) + gated(1, r, k) + gated(3, r, k)
            return 0
        lax.fori_loop(begin, end, body, 0)

    def add_two_hop(k, i, r):
        acc[k][:, i] = acc[k][:, i] + gated(2, r, k)
        if i == 0:
            far.append(rcopy(acc[k].at[1, pl.ds(0, 1)], d2d[k].at[pl.ds(0, 1)], partner))
            far[k].start()
        if i == side - 1:
            near.append(rcopy(acc[k].at[1, pl.ds(1, side - 1)], d2d[k].at[pl.ds(1, side - 1)], partner))
            near[k].start()

    def stage_far(k):
        far[k].wait_recv()
        acc[k][0, 0] = acc[k][0, 0] + d2d[k][0]
        t_p.append(rcopy(acc[k].at[0, 0, lo_t], tpl[k], xp))
        t_m.append(rcopy(acc[k].at[0, 0, hi_t], tmi[k], xm))
        t_p[k].start()
        t_m[k].start()

    def stage_near(k):
        near[k].wait_recv()
        for i in range(1, side):
            acc[k][0, i] = acc[k][0, i] + d2d[k][i]

    def stage_c(k):
        t_p[k].wait_recv()
        acc[k][0, 1, lo_t] = acc[k][0, 1, lo_t] + tpl[k][...]
        r_p.append(rcopy(acc[k].at[0, 1], rpl[k], xp))
        r_p[k].start()
        t_m[k].wait_recv()
        acc[k][0, 2, hi_t] = acc[k][0, 2, hi_t] + tmi[k][...]
        r_m.append(rcopy(acc[k].at[0, 2], rmi[k], xm))
        r_m[k].start()

    def stage_d(k):
        r_p[k].wait_recv()
        r_m[k].wait_recv()
        c0, cw = cols[k]
        total = xbuf[0, 0, :, c0:c0 + cw].astype(F32) + acc[k][0, 3]
        out_ref[:, c0:c0 + cw] = (total + rpl[k][...] + rmi[k][...]).astype(BF16)

    blocks = ((0, 2), (1, 1), (2, 3), (3, 0))
    for k in range(min(2, n_chunk)):
        forward(k)
    first(0, 0, side)
    for p, q in enumerate(pieces[:-1]):
        wgt_2[p].wait_recv()
        wup_2[p].wait_recv()
        h_all(2, q)
    wgt_2[-1].wait_recv()
    wup_2[-1].wait_recv()
    for i, r in blocks:
        h_row(2, r, pieces[-1])
        if i == 0:
            arrive(hop[0])
        add_two_hop(0, i, r)
        if i == 2:
            stage_far(0)
    for k in range(n_chunk):
        if k > 0:
            arrive(hop[k])
            for i, r in blocks:
                add_two_hop(k, i, r)
        if k + 1 < n_chunk:
            first(k + 1, 0, MID)
        if k > 0:
            stage_far(k)
        if k > 1:
            stage_c(k - 1)
        if k + 2 < n_chunk:
            forward(k + 2)
        if k + 1 < n_chunk:
            first(k + 1, MID, side)
        stage_near(k)
        if k == 0 and n_chunk > 1:
            stage_c(0)
        if k >= 2:
            stage_d(k - 2)
    stage_c(n_chunk - 1)
    for k in range(max(n_chunk - 2, 0), n_chunk):
        stage_d(k)
    for c in sent:
        c.wait_send()


def solution(mesh):
    group_size = mesh.shape["ep"]
    side = math.isqrt(group_size // CORES)
    row_spec = P(("dp", "ep"))

    def local_step(tokens, expert_ids, gate_w, route_counts, w_gate, w_up, w_down):
        tok_n, dim = tokens.shape
        ffn = w_gate.shape[2]
        n_exp = route_counts.shape[1]
        widths = CHUNKS if sum(CHUNKS) == dim else (LANES,) * (dim // LANES)
        cols = tuple((sum(widths[:k]), cw) for k, cw in enumerate(widths))
        n_copy = 5 + 4 + 4 + 3 + 3 + 2 * PIECES + 12 * len(cols)
        vmem = pl.BlockSpec(memory_space=pltpu.VMEM)
        anym = pl.BlockSpec(memory_space=pl.ANY)
        return pl.pallas_call(
            lambda *refs: call_kernel(side, cols, refs),
            out_shape=pltpu.VMEM((tok_n, dim), BF16),
            in_specs=[vmem] * 3 + [anym] * 4,
            out_specs=vmem,
            scratch_shapes=[
                pltpu.VMEM((side, CORES, tok_n, dim), BF16),
                pltpu.VMEM((side, CORES, n_exp, tok_n), F32),
                pltpu.VMEM((side, side, CORES, tok_n, LANES), F32),
                pltpu.VMEM((side, dim, ffn), BF16),
                pltpu.VMEM((side, dim, ffn), BF16),
                pltpu.VMEM((side, side, CORES, tok_n, ffn), BF16),
                [pltpu.VMEM((side, ffn, cw), BF16) for _, cw in cols],
                [pltpu.VMEM((CORES, side, tok_n, cw), F32) for _, cw in cols],
                [pltpu.VMEM((side, tok_n, cw), F32) for _, cw in cols],
                [pltpu.VMEM((tok_n // 2, cw), F32) for _, cw in cols],
                [pltpu.VMEM((tok_n // 2, cw), F32) for _, cw in cols],
                [pltpu.VMEM((tok_n, cw), F32) for _, cw in cols],
                [pltpu.VMEM((tok_n, cw), F32) for _, cw in cols],
                pltpu.SemaphoreType.DMA((n_copy,)),
                pltpu.SemaphoreType.DMA((n_copy,)),
                pltpu.SemaphoreType.DMA((3 + len(cols),)),
            ],
            compiler_params=pltpu.CompilerParams(collective_id=0, has_side_effects=True, vmem_limit_bytes=60 * 2 ** 20),
            name="moe_kernel",
        )(expert_ids.T, gate_w.T, route_counts, tokens, w_gate, w_up, w_down)

    def call_kernel(side, cols, refs):
        moe_kernel(side, cols, *refs)

    return jax.shard_map(local_step, mesh=mesh, in_specs=(row_spec, row_spec, row_spec, row_spec, P("ep"), P("ep"), P("ep")), out_specs=row_spec, check_vma=False)
```
